768 devices in a mesh: dom: 64 (over y, x, core), sub: 12 (over z).
Axes of the slice: x: 4, y: 8, z: 12, core: 2. Of those that a mesh axis runs over, the one named last changes fastest.
Arguments:
- dof_values: float32 [56, 9, 98304], P(None, None, ('dom', 'sub')), may hold values from -0.6 to 0.6
- stiffness: float32 [3, 56, 56], replicated, may hold values from -0.75 to 0.75
- face_project: float32 [4, 21, 56], replicated, may hold values from -0.75 to 0.75
- face_lift: float32 [4, 56, 21], replicated, may hold values from -1.25 to 1.25
- face_rotate: float32 [3, 21, 21], replicated, may hold values from -1.25 to 1.25
- star_matrices: float32 [3, 9, 9, 98304], P(None, None, None, ('dom', 'sub')), may hold values from -2 to 2
- flux_local: float32 [4, 9, 9, 98304], P(None, None, None, ('dom', 'sub')), may hold values from -1.2 to 1.2
- flux_neighbour: float32 [4, 9, 9, 98304], P(None, None, None, ('dom', 'sub')), may hold values from -1.2 to 1.2
- cluster_labels: int32 [98304], P(('dom', 'sub')), may hold values from 0 to 1, as said below
- neighbour_index: int32 [4, 98304], P(None, ('dom', 'sub')), may hold values from 0 to 351, as said below
- neighbour_face: int32 [4, 98304], P(None, ('dom', 'sub')), may hold values from 0 to 3
- neighbour_orient: int32 [4, 98304], P(None, ('dom', 'sub')), may hold values from 0 to 2
- send_element: int32 [768, 224], P(('dom', 'sub')), may hold values from 0 to 127
- send_face: int32 [768, 224], P(('dom', 'sub')), may hold values from 0 to 3
Outputs:
- new_dofs: float32 [56, 9, 98304], P(None, None, ('dom', 'sub'))
The draws below stay inside these ranges and needn't reach their ends.
Inputs may be any that keep to these rules, and one draw needn't show every extreme that they name: `cluster_labels`: 0 marks an element of the fine cluster, 1 of the coarse cluster. `neighbour_index`: values below 128 name an own element of the same device; value 128 + s names receive slot s of that device. Every receive slot of a device is named by exactly one face of that device's elements.
All inputs are finite; a program needn't handle non-finite values.
Results may differ from the reference program's by a relative error of at most 0.0001.
Values sent between devices are 32-bit elements; how exact they have to be, the bound alone decides.
A program may use at most 128 MiB of HBM per device.

```python
import jax
import jax.numpy as jnp
from jax import lax

BASIS = 56
FACE_BASIS = 21
QUANTITIES = 9
TAYLOR_TERMS = 6
ELEMENTS_DEV = 128
HALO_CURVE = 64
HALO_PEER = 8
HALO_SLOTS = 224
ELEMENTS = 98304
N_DOM = 64
N_SUB = 12
DEVICES = 768


def draw_cluster_labels(key, part):
    devices = ELEMENTS // ELEMENTS_DEV
    share = jax.random.randint(jax.random.fold_in(key, 11), (devices, 1), 10, 71)
    rolls = jax.random.randint(jax.random.fold_in(key, 12), (devices, ELEMENTS_DEV), 0, 100)
    return (rolls >= share).astype(jnp.int32).reshape(ELEMENTS)


def draw_neighbour_index(key, part):
    devices = ELEMENTS // ELEMENTS_DEV
    device_keys = jax.random.split(jax.random.fold_in(key, 21), devices)

    def one_device(device_key):
        shuffled = jax.random.permutation(jax.random.fold_in(device_key, 1), 4 * ELEMENTS_DEV).astype(jnp.int32)
        locals_drawn = jax.random.randint(jax.random.fold_in(device_key, 2), (4 * ELEMENTS_DEV,), 0, ELEMENTS_DEV)
        return jnp.where(shuffled < HALO_SLOTS, ELEMENTS_DEV + shuffled, locals_drawn).astype(jnp.int32)
    table = jax.vmap(one_device)(device_keys)
    return jnp.transpose(table.reshape(devices, 4, ELEMENTS_DEV), (1, 0, 2)).reshape(4, ELEMENTS)


def place_ends(drawn, key, least, high):
    longest = drawn.shape.index(max(drawn.shape))
    spots = []
    for shift in (0, 1):
        where = [jax.random.randint(jax.random.fold_in(key, axis), (), 0, length) for axis, length in enumerate(drawn.shape)]
        where[longest] = (where[longest] + shift) % drawn.shape[longest]
        spots.append(tuple(where))
    return drawn.at[spots[0]].set(least).at[spots[1]].set(high)


def block_levels(rng, dims, cuts, smallest, top_value):
    factor_of = 1.0
    for axis_at, parts in cuts:
        heights = jax.random.uniform(jax.random.fold_in(jax.random.fold_in(rng, 6), axis_at), (parts,), jnp.float32, smallest / len(cuts), top_value / len(cuts))
        factor_of = factor_of * jnp.repeat(jnp.exp(heights), dims[axis_at] // parts).reshape((-1,) + (1,) * (len(dims) - 1 - axis_at))
    return factor_of


def noise(own_key, shape, scale, reach, cuts=(), kind=jnp.bfloat16):
    array = scale * jax.random.normal(own_key, shape, jnp.float32)
    if cuts:
        array = array * block_levels(own_key, shape, cuts, -0.22, 0.18)
    return jnp.clip(array, -reach, reach).astype(kind)


def setup_inputs(seed: int = 0) -> dict:
    key_of = jax.random.split(jax.random.key(seed), 15)
    return {
        "dof_values": noise(key_of[0], (BASIS, QUANTITIES, ELEMENTS), 0.1, 0.6, ((2, 768),), jnp.float32),
        "stiffness": noise(key_of[1], (3, BASIS, BASIS), BASIS ** -0.5, 0.75, (), jnp.float32),
        "face_project": noise(key_of[2], (4, FACE_BASIS, BASIS), BASIS ** -0.5, 0.75, (), jnp.float32),
        "face_lift": noise(key_of[3], (4, BASIS, FACE_BASIS), FACE_BASIS ** -0.5, 1.25, (), jnp.float32),
        "face_rotate": noise(key_of[4], (3, FACE_BASIS, FACE_BASIS), FACE_BASIS ** -0.5, 1.25, (), jnp.float32),
        "star_matrices": noise(key_of[5], (3, QUANTITIES, QUANTITIES, ELEMENTS), 0.33, 2.0, ((3, 768),), jnp.float32),
        "flux_local": noise(key_of[6], (4, QUANTITIES, QUANTITIES, ELEMENTS), 0.2, 1.2, ((3, 768),), jnp.float32),
        "flux_neighbour": noise(key_of[7], (4, QUANTITIES, QUANTITIES, ELEMENTS), 0.2, 1.2, ((3, 768),), jnp.float32),
        "cluster_labels": draw_cluster_labels(jax.random.fold_in(key_of[14], 71), 0),
        "neighbour_index": draw_neighbour_index(jax.random.fold_in(key_of[14], 71), 0),
        "neighbour_face": place_ends(jax.random.randint(key_of[10], (4, ELEMENTS), 0, 4), jax.random.fold_in(key_of[10], 1), 0, 3).astype(jnp.int32),
        "neighbour_orient": place_ends(jax.random.randint(key_of[11], (4, ELEMENTS), 0, 3), jax.random.fold_in(key_of[11], 1), 0, 2).astype(jnp.int32),
        "send_element": place_ends(jax.random.randint(key_of[12], (DEVICES, HALO_SLOTS), 0, ELEMENTS_DEV), jax.random.fold_in(key_of[12], 1), 0, ELEMENTS_DEV - 1).astype(jnp.int32),
        "send_face": place_ends(jax.random.randint(key_of[13], (DEVICES, HALO_SLOTS), 0, 4), jax.random.fold_in(key_of[13], 1), 0, 3).astype(jnp.int32),
    }


highest = lax.Precision.HIGHEST
step_fine = 1.0


def left_apply(matrix, values):
    rows = values.shape[0]
    flat = values.reshape(rows, -1)
    out = jnp.dot(matrix, flat, precision=highest, preferred_element_type=jnp.float32)
    return out.reshape((matrix.shape[0],) + values.shape[1:])


def mix_variables(values, mats):
    running = values[:, 0, None, :] * mats[0][None, :, :]
    for inner in range(1, values.shape[1]):
        running = running + values[:, inner, None, :] * mats[inner][None, :, :]
    return running


def derive(values, stiffness, star_matrices):
    running = None
    for direction in range(3):
        spread = left_apply(jnp.transpose(stiffness[direction]), values)
        term = mix_variables(spread, star_matrices[direction])
        running = term if running is None else running + term
    return running


def volume_part(values, stiffness, star_matrices):
    running = None
    for direction in range(3):
        spread = left_apply(stiffness[direction], values)
        term = mix_variables(spread, star_matrices[direction])
        running = term if running is None else running + term
    return running


def time_integrals(values, stiffness, star_matrices, intervals):
    running = [jnp.zeros_like(values) for interval in intervals]
    derivative = values
    factor = 1.0
    for degree in range(TAYLOR_TERMS):
        factor = factor * (degree + 1)
        running = [total + ((interval[1] ** (degree + 1) - interval[0] ** (degree + 1)) / factor) * derivative
                   for total, interval in zip(running, intervals)]
        if degree + 1 < TAYLOR_TERMS:
            derivative = derive(derivative, stiffness, star_matrices)
    return running


def face_traces(integral, face_project):
    fbasis = face_project.shape[1]
    stacked = left_apply(face_project.reshape(4 * fbasis, face_project.shape[2]), integral)
    stacked = stacked.reshape(4, fbasis, integral.shape[1], integral.shape[2])
    return jnp.transpose(stacked, (1, 2, 0, 3))


def chosen_traces(integral, chosen_elements, chosen_faces, face_project):
    picked = integral[:, :, chosen_elements]
    fbasis = face_project.shape[1]
    every = left_apply(face_project.reshape(4 * fbasis, face_project.shape[2]), picked)
    every = every.reshape(4, fbasis, picked.shape[1], picked.shape[2])
    select = (chosen_faces[None, :] == jnp.arange(4, dtype=jnp.int32)[:, None]).astype(every.dtype)
    return jnp.sum(every * select[:, None, None, :], axis=0)


def flux_sum(traces, face_lift, solvers):
    solved = jnp.stack([mix_variables(traces[:, :, face, :], solvers[face]) for face in range(4)], axis=0)
    fbasis = face_lift.shape[2]
    lift_all = jnp.transpose(face_lift, (1, 0, 2)).reshape(face_lift.shape[1], 4 * fbasis)
    return left_apply(lift_all, solved.reshape((4 * fbasis,) + solved.shape[2:]))


def rotate(traces, neighbour_orient, face_rotate):
    rotated = jnp.zeros_like(traces)
    for variant in range(3):
        chosen = (neighbour_orient == variant)[None, None, :, :]
        turned = left_apply(face_rotate[variant], traces)
        rotated = rotated + jnp.where(chosen, turned, jnp.zeros_like(turned))
    return rotated


def residual_update(integral, traces, stiffness, star_matrices, face_project, face_lift, face_rotate,
                    flux_local, flux_neighbour, neighbour_orient):
    volume = volume_part(integral, stiffness, star_matrices)
    own_flux = flux_sum(face_traces(integral, face_project), face_lift, flux_local)
    remote = flux_sum(rotate(traces, neighbour_orient, face_rotate), face_lift, flux_neighbour)
    return volume - own_flux - remote


def neighbour_traces(integral, face_project, neighbour_index, neighbour_face, send_element, send_face):
    width = integral.shape[1]
    fbasis = face_project.shape[1]
    own_all = face_traces(integral, face_project)
    owners = jnp.arange(DEVICES, dtype=jnp.int32)[:, None] * ELEMENTS_DEV
    global_elements = (owners + send_element).reshape(-1)
    sent = chosen_traces(integral, global_elements, send_face.reshape(-1), face_project)
    sent = sent.reshape(fbasis, width, N_DOM, N_SUB, HALO_SLOTS)
    blank = jnp.zeros((fbasis, width, 1, N_SUB, HALO_CURVE), sent.dtype)
    from_below = jnp.concatenate([blank, sent[:, :, :-1, :, HALO_CURVE:2 * HALO_CURVE]], axis=2)
    from_above = jnp.concatenate([sent[:, :, 1:, :, 0:HALO_CURVE], blank], axis=2)
    peers = sent[:, :, :, :, 2 * HALO_CURVE:].reshape(fbasis, width, N_DOM, N_SUB, N_SUB, HALO_PEER)
    peers = jnp.swapaxes(peers, 3, 4).reshape(fbasis, width, N_DOM, N_SUB, N_SUB * HALO_PEER)
    received = jnp.concatenate([from_below, from_above, peers], axis=4).reshape(fbasis, width, DEVICES * HALO_SLOTS)
    table = jnp.concatenate([own_all.reshape(fbasis, width, 4 * ELEMENTS), received], axis=2)
    device_of = (jnp.arange(ELEMENTS, dtype=jnp.int32) // ELEMENTS_DEV)[None, :]
    lookup = jnp.where(neighbour_index < ELEMENTS_DEV,
                       neighbour_face * ELEMENTS + device_of * ELEMENTS_DEV + neighbour_index,
                       4 * ELEMENTS + device_of * HALO_SLOTS + neighbour_index - ELEMENTS_DEV).astype(jnp.int32)
    return table[:, :, lookup]


def reference(dof_values, stiffness, face_project, face_lift, face_rotate, star_matrices, flux_local,
              flux_neighbour, cluster_labels, neighbour_index, neighbour_face, neighbour_orient,
              send_element, send_face):
    fine_mask = (cluster_labels == 0)[None, None, :]
    first, second = time_integrals(dof_values, stiffness, star_matrices,
                                   [(0.0, step_fine), (step_fine, 2.0 * step_fine)])
    traces_one = neighbour_traces(first, face_project, neighbour_index, neighbour_face, send_element, send_face)
    update_one = residual_update(first, traces_one, stiffness, star_matrices, face_project, face_lift,
                                 face_rotate, flux_local, flux_neighbour, neighbour_orient)
    middle = jnp.where(fine_mask, dof_values + update_one, dof_values)
    restart = time_integrals(middle, stiffness, star_matrices, [(0.0, step_fine)])[0]
    later = jnp.where(fine_mask, restart, second)
    traces_two = neighbour_traces(later, face_project, neighbour_index, neighbour_face, send_element, send_face)
    own_integral = jnp.where(fine_mask, later, first + second)
    fine_faces = fine_mask[:, :, None, :]
    all_traces = jnp.where(fine_faces, traces_two, traces_one + traces_two)
    start_state = jnp.where(fine_mask, middle, dof_values)
    update_two = residual_update(own_integral, all_traces, stiffness, star_matrices, face_project, face_lift,
                                 face_rotate, flux_local, flux_neighbour, neighbour_orient)
    return start_state + update_two
```

```python
import functools

import jax
import jax.numpy as jnp
from jax import lax
from jax.experimental import pallas as pl
from jax.experimental.pallas import tpu as pltpu
from jax.sharding import PartitionSpec as P

MESH = pl.DeviceIdType.MESH
F32, BF16 = jnp.float32, jnp.bfloat16
HIGHEST = lax.Precision.HIGHEST

NB = 56
NBP = 64
NQ = 9
NE = 128
NM = 21
NMP = 24
CURVE = 64
PEER = 8
TERMS = 6
LANES = NQ * NE
TRACE = 224
TRACEP = 256

NN = (((1,), (0,)), ((), ()))
NT = (((1,), (1,)), ((), ()))
TN = (((0,), (0,)), ((), ()))


def mm(a, b, dims=NN):
    return lax.dot_general(a, b, dims, preferred_element_type=F32)


def mm_exact(a, b, dims=NN):
    return lax.dot_general(a, b, dims, precision=HIGHEST, preferred_element_type=F32)


def iota(shape, dim):
    return lax.broadcasted_iota(jnp.int32, shape, dim)


def split(x):
    hi = x.astype(BF16)
    lo = (x - hi.astype(F32)).astype(BF16)
    return hi, lo


def row_block(index):
    out = jnp.zeros_like(index)
    for k in range(1, NQ):
        out = out + (index >= NMP * k).astype(jnp.int32)
    return out


def col(v):
    return slice(v * NE, (v + 1) * NE)


def kernel(
    nd, ns,
    dof_hbm, star_hbm, fluxl_hbm, fluxn_hbm,
    stiff, proj, lift, rot, labels, nidx, nface, norient, selem, sface,
    out,
    dof, star, fluxl, fluxn, starb, fluxlb, fluxnb,
    ader, avol, pst, lst, krc, tall,
    x, i1, i2, xs, z, vol, pi1, pi, t2, t2m, ohs, ohr, oho, zown, zr1, sol, rotm,
    send, recv,
    in_sem, send_sem, recv_sem,
):
    a = lax.axis_index("dom")
    b = lax.axis_index("sub")
    nslots = 2 * CURVE + PEER * ns

    barrier = pltpu.get_barrier_semaphore()

    @pl.when(a > 0)
    def _():
        pl.semaphore_signal(barrier, inc=1, device_id=(a - 1, b), device_id_type=MESH)

    @pl.when(a < nd - 1)
    def _():
        pl.semaphore_signal(barrier, inc=1, device_id=(a + 1, b), device_id_type=MESH)

    for o in range(1, ns):
        pl.semaphore_signal(barrier, inc=1, device_id=(a, lax.rem(b + o, ns)), device_id_type=MESH)

    copies = [
        pltpu.make_async_copy(src, dst, in_sem.at[k])
        for k, (src, dst) in enumerate(
            [(dof_hbm, dof), (star_hbm, star), (fluxl_hbm, fluxl), (fluxn_hbm, fluxn)]
        )
    ]
    for c in copies:
        c.start()

    def stacked(w):
        hi, lo = split(w)
        lane = iota(w.shape, 1)
        return jnp.where(lane < 2 * NBP, hi.astype(F32), lo.astype(F32)).astype(BF16)

    lane = iota((NB, 3 * NBP), 1)
    lane = lane - NBP * ((lane >= NBP).astype(jnp.int32) + (lane >= 2 * NBP).astype(jnp.int32))
    eye3 = (lane == iota((NB, 3 * NBP), 0)).astype(F32)

    def build_map(target, dims):
        tall[...] = jnp.zeros_like(tall)
        for d in range(3):
            tall[d * NB : (d + 1) * NB, :] = mm_exact(stiff[d], eye3, dims)
        target[...] = stacked(tall[0:176, :])

    build_map(ader, TN)
    for f in range(4):
        pi[f * NMP : (f + 1) * NMP, :] = jnp.zeros((NMP, LANES), F32)
        pi[f * NMP : f * NMP + NM, 0:NB] = proj[:, f, :]
    pst[...] = stacked(mm_exact(pi[0:96, 0:NB], eye3))

    ohs[...] = jnp.zeros_like(ohs)
    diagonal = iota((nslots, nslots), 0) == iota((nslots, nslots), 1)
    ones = jnp.ones((nslots, NE), BF16)

    def as_column(row):
        spread = jnp.where(diagonal, jnp.broadcast_to(row.astype(F32), diagonal.shape), 0.0)
        return mm(spread.astype(BF16), ones)

    elem_col = as_column(selem[...])
    face_col = as_column(sface[...])
    lane_e = iota((nslots, NE), 1).astype(F32)
    for f in range(4):
        pick = (elem_col == lane_e) & (face_col == float(f))
        ohs[0:nslots, col(f)] = pick.astype(F32).astype(BF16)

    blank = jnp.zeros((CURVE, TRACEP), F32)
    for ex in range(2):
        @pl.when(a == 0)
        def _():
            recv[ex, 0:CURVE, :] = blank

        @pl.when(a == nd - 1)
        def _():
            recv[ex, CURVE : 2 * CURVE, :] = blank

        recv[ex, nslots:, :] = jnp.zeros((recv.shape[1] - nslots, TRACEP), F32)

    t2[...] = jnp.zeros_like(t2)
    x[NB:, :] = jnp.zeros((NBP - NB, LANES), F32)
    i1[NB:, :] = jnp.zeros((NBP - NB, LANES), F32)
    i2[NB:, :] = jnp.zeros((NBP - NB, LANES), F32)

    copies[0].wait()
    copies[1].wait()
    for v in range(NQ):
        for w in range(NQ):
            for d in range(3):
                starb[v, w, d] = jnp.broadcast_to(star[v, w, d : d + 1, :], (8, NE))

    def load_xs(value):
        hi, lo = split(value)
        xs[0:NBP, :] = hi
        xs[NBP : 2 * NBP, :] = lo
        xs[2 * NBP : 3 * NBP, :] = hi

    def mapped(matrix, target):
        z[...] = mm(matrix[...], xs[...])
        for w0 in range(0, NQ, 3):
            acc = [None, None, None]
            for v in range(NQ):
                for d in range(3):
                    zb = z[d * NB : (d + 1) * NB, col(v)].reshape(NB // 8, 8, NE)
                    for k in range(3):
                        term = zb * starb[v, w0 + k, d][None]
                        acc[k] = term if acc[k] is None else acc[k] + term
            for k in range(3):
                target[0:NB, col(w0 + k)] = acc[k].reshape(NB, NE)

    first_c, second_c = [1.0], [1.0]
    fact = 1.0
    for k in range(1, TERMS):
        fact *= k + 1
        first_c.append(1.0 / fact)
        second_c.append((2.0 ** (k + 1) - 1.0) / fact)

    def coefficient(k, table):
        out_c = jnp.float32(table[-1])
        for j in range(TERMS - 2, 0, -1):
            out_c = jnp.where(k == j, jnp.float32(table[j]), out_c)
        return out_c

    fine_row = labels[...] == 0
    fine = jnp.broadcast_to(fine_row, (NB, NE))

    for v in range(NQ):
        x[0:NB, col(v)] = dof[v]
    i1[...] = x[...]
    i2[...] = x[...]

    def step_one(k, carry):
        load_xs(x[...])
        mapped(ader, x)
        i1[...] = i1[...] + coefficient(k, first_c) * x[...]
        i2[...] = i2[...] + coefficient(k, second_c) * x[...]
        return carry

    lax.fori_loop(1, TERMS, step_one, 0)

    def project(integral):
        load_xs(integral)
        pi[...] = mm(pst[...], xs[...])
        for f in range(4):
            for v in range(NQ):
                t2[v * NMP : (v + 1) * NMP, col(f)] = pi[f * NMP : (f + 1) * NMP, col(v)]
        hi, lo = split(t2[...])
        t2m[0:TRACEP, :] = hi
        t2m[TRACEP:, :] = lo

    def curve_copy(ex, up):
        src = pl.ds(CURVE if up else 0, CURVE)
        dst = pl.ds(0 if up else CURVE, CURVE)
        return pltpu.make_async_remote_copy(
            src_ref=send.at[ex, src, :],
            dst_ref=recv.at[ex, dst, :],
            send_sem=send_sem.at[ex, 0 if up else 1],
            recv_sem=recv_sem.at[ex, 0 if up else 1],
            device_id=(a + 1 if up else a - 1, b),
            device_id_type=MESH,
        )

    def peer_rows(p):
        return pl.ds(pl.multiple_of(2 * CURVE + p * PEER, PEER), PEER)

    def peer_copy(ex, p, source):
        return pltpu.make_async_remote_copy(
            src_ref=send.at[ex, peer_rows(p), :],
            dst_ref=recv.at[ex, peer_rows(source), :],
            send_sem=send_sem.at[ex, 2 + p],
            recv_sem=recv_sem.at[ex, 2 + source],
            device_id=(a, p),
            device_id_type=MESH,
        )

    order = sorted(range(1, ns), key=lambda o: -min(o, ns - o))

    def start_exchange(ex):
        both = mm(ohs[...], t2m[...], NT)
        send[ex] = both[:, 0:TRACEP] + both[:, TRACEP:]
        if ex == 0:
            count = ns - 1 + (a > 0).astype(jnp.int32) + (a < nd - 1).astype(jnp.int32)
            pl.semaphore_wait(barrier, count)
        for o in order:
            p = lax.rem(b + o, ns)
            peer_copy(ex, p, b).start()

        @pl.when(a < nd - 1)
        def _():
            curve_copy(ex, True).start()

        @pl.when(a > 0)
        def _():
            curve_copy(ex, False).start()

        recv[ex, peer_rows(b), :] = send[ex, peer_rows(b), :]

    def finish_exchange(ex):
        @pl.when(a > 0)
        def _():
            curve_copy(ex, True).wait_recv()

        @pl.when(a < nd - 1)
        def _():
            curve_copy(ex, False).wait_recv()

        for o in order:
            p = lax.rem(b + o, ns)
            peer_copy(ex, p, p).wait_recv()

    def finish_sends(ex):
        @pl.when(a < nd - 1)
        def _():
            curve_copy(ex, True).wait_send()

        @pl.when(a > 0)
        def _():
            curve_copy(ex, False).wait_send()

        for o in order:
            p = lax.rem(b + o, ns)
            peer_copy(ex, p, p).wait_send()

    def rotated_own(slot):
        picked = mm(t2m[...], oho[...])
        picked = picked[0:TRACEP, :] + picked[TRACEP:, :]
        hi, lo = split(picked)
        turned = mm(krc[...], jnp.concatenate([hi, lo, hi], axis=0))
        for f in range(4):
            orient = norient[f : f + 1, :]
            pick = jnp.where(
                orient == 0,
                turned[0:TRACE, col(f)],
                jnp.where(orient == 1, turned[TRACE : 2 * TRACE, col(f)], turned[2 * TRACE :, col(f)]),
            )
            if slot == 1:
                pick = pick + jnp.where(fine_row, 0.0, zr1[:, col(f)])
            zown[:, col(f)] = pick

    def local_flux():
        for f in range(4):
            for w0 in range(0, NQ, 3):
                acc = [None, None, None]
                for v in range(NQ):
                    block = pi[f * NMP : (f + 1) * NMP, col(v)].reshape(NMP // 8, 8, NE)
                    for k in range(3):
                        term = block * fluxlb[v, w0 + k, f][None]
                        acc[k] = term if acc[k] is None else acc[k] + term
                for k in range(3):
                    sol[f * NMP : (f + 1) * NMP, col(w0 + k)] = acc[k].reshape(NMP, NE)

    def remote_flux(slot_orient, ex):
        hi, lo = split(recv[ex])
        turned = mm(krc[...], jnp.concatenate([hi, lo, hi], axis=1), NT)
        pick = jnp.where(
            slot_orient < 0.5,
            turned[0:TRACE],
            jnp.where(slot_orient < 1.5, turned[TRACE : 2 * TRACE], turned[2 * TRACE :]),
        )
        hi, lo = split(pick)
        rotm[0:TRACE, :] = hi
        rotm[TRACE:, :] = lo
        arrived = mm(rotm[...], ohr[...])
        zown[...] = zown[...] + arrived[0:TRACE] + arrived[TRACE:]
        for f in range(4):
            for w0 in range(0, NQ, 3):
                acc = [
                    sol[f * NMP : (f + 1) * NMP, col(w0 + k)].reshape(NMP // 8, 8, NE) for k in range(3)
                ]
                for v in range(NQ):
                    block = zown[v * NMP : (v + 1) * NMP, col(f)].reshape(NMP // 8, 8, NE)
                    for k in range(3):
                        acc[k] = acc[k] + block * fluxnb[v, w0 + k, f][None]
                for k in range(3):
                    sol[f * NMP : (f + 1) * NMP, col(w0 + k)] = acc[k].reshape(NMP, NE)
        hi, lo = split(sol[...])
        lifted = mm(lst[...], jnp.concatenate([hi, lo], axis=0))
        vol[...] = vol[...] - lifted[0:NB] - lifted[NBP : NBP + NB]

    project(i1[...])
    start_exchange(0)

    build_map(avol, NN)
    copies[2].wait()
    copies[3].wait()
    for v in range(NQ):
        for w in range(NQ):
            for f in range(4):
                fluxlb[v, w, f] = jnp.broadcast_to(fluxl[v, w, f : f + 1, :], (8, NE))
                fluxnb[v, w, f] = jnp.broadcast_to(fluxn[v, w, f : f + 1, :], (8, NE))

    tall[...] = jnp.zeros_like(tall)
    for f in range(4):
        tall[f * NMP : f * NMP + NM, 0:NB] = lift[:, f, :]
    lane2 = iota((96, 192), 1)
    lane2 = lane2 - 96 * (lane2 >= 96).astype(jnp.int32)
    eye2 = (lane2 == iota((96, 192), 0)).astype(F32)
    wide = mm_exact(tall[0:96, 0:NBP], eye2, TN)
    hi, lo = split(wide)
    lst[0:NBP, :] = hi
    lst[NBP:, :] = lo

    rows = iota((TRACEP, NM), 0)
    tile_of = ((rows - NMP * row_block(rows)) == iota((TRACEP, NM), 1)).astype(F32)
    tile_of = jnp.where(rows < NQ * NMP, tile_of, 0.0)
    same = row_block(iota((TRACE, TRACEP), 0)) == row_block(iota((TRACE, TRACEP), 1))
    for o in range(3):
        turned = mm_exact(tile_of[0:TRACE], rot[o])
        turned = jnp.where(same, mm_exact(turned, tile_of, NT), 0.0)
        hi, lo = split(turned)
        here = slice(o * TRACE, (o + 1) * TRACE)
        krc[here, 0:TRACEP] = hi
        krc[here, TRACEP : 2 * TRACEP] = hi
        krc[here, 2 * TRACEP :] = lo

    nslot_rows = ohr.shape[0]
    for f in range(4):
        index = nidx[f : f + 1, :]
        ohr[:, col(f)] = (iota((nslot_rows, NE), 0) + NE == index).astype(F32).astype(BF16)
        own = jnp.where(index < NE, nface[f : f + 1, :] * NE + index, -1)
        oho[:, col(f)] = (iota((4 * NE, NE), 0) == own).astype(F32).astype(BF16)

    slot_orient = mm(
        jnp.concatenate(
            [jnp.broadcast_to(norient[f : f + 1, :].astype(F32), (16, NE)) for f in range(4)], axis=1
        ).astype(BF16),
        ohr[...],
        NT,
    )[0:1, :]

    rotated_own(0)
    local_flux()
    pi1[...] = pi[...]
    mapped(avol, vol)

    finish_exchange(0)
    remote_flux(slot_orient, 0)
    zr1[...] = zown[...]

    for v in range(NQ):
        x[0:NB, col(v)] = dof[v] + jnp.where(fine, vol[:, col(v)], 0.0)
        dof[v] = x[0:NB, col(v)]
    t = x[...]
    z[0:NBP, :] = t

    def step_two(k, carry):
        load_xs(x[...])
        mapped(ader, x)
        vol[...] = vol[...] + coefficient(k, first_c) * x[0:NB, :]
        return carry

    vol[...] = t[0:NB]
    lax.fori_loop(1, TERMS, step_two, 0)
    for v in range(NQ):
        later = jnp.where(fine, vol[:, col(v)], i2[0:NB, col(v)])
        i1[0:NB, col(v)] = later + jnp.where(fine, 0.0, i1[0:NB, col(v)])
        i2[0:NB, col(v)] = later

    project(i2[...])
    start_exchange(1)

    for v in range(NQ):
        pi[:, col(v)] = pi[:, col(v)] + jnp.where(fine_row, 0.0, pi1[:, col(v)])
    rotated_own(1)
    local_flux()
    load_xs(i1[...])
    mapped(avol, vol)

    finish_exchange(1)
    remote_flux(slot_orient, 1)
    for v in range(NQ):
        out[v] = dof[v] + vol[:, col(v)]
    finish_sends(0)
    finish_sends(1)


def solution(mesh):
    nd, ns = mesh.shape["dom"], mesh.shape["sub"]
    nslots = 2 * CURVE + PEER * ns
    nslots_pad = -(-nslots // 128) * 128

    def per_device(
        dof_values, stiffness, face_project, face_lift, face_rotate, star_matrices,
        flux_local, flux_neighbour, cluster_labels, neighbour_index, neighbour_face,
        neighbour_orient, send_element, send_face,
    ):
        hbm = pl.BlockSpec(memory_space=pl.ANY)
        vmem = pl.BlockSpec(memory_space=pltpu.VMEM)
        scratch = [
            pltpu.VMEM((NQ, NB, NE), F32),
            pltpu.VMEM((NQ, NQ, 3, NE), F32),
            pltpu.VMEM((NQ, NQ, 4, NE), F32),
            pltpu.VMEM((NQ, NQ, 4, NE), F32),
            pltpu.VMEM((NQ, NQ, 3, 8, NE), F32),
            pltpu.VMEM((NQ, NQ, 4, 8, NE), F32),
            pltpu.VMEM((NQ, NQ, 4, 8, NE), F32),
            pltpu.VMEM((176, 3 * NBP), BF16),
            pltpu.VMEM((176, 3 * NBP), BF16),
            pltpu.VMEM((96, 3 * NBP), BF16),
            pltpu.VMEM((2 * NBP, 192), BF16),
            pltpu.VMEM((3 * TRACE, 3 * TRACEP), BF16),
            pltpu.VMEM((176, 3 * NBP), F32),
            pltpu.VMEM((NBP, LANES), F32),
            pltpu.VMEM((NBP, LANES), F32),
            pltpu.VMEM((NBP, LANES), F32),
            pltpu.VMEM((3 * NBP, LANES), BF16),
            pltpu.VMEM((176, LANES), F32),
            pltpu.VMEM((NB, LANES), F32),
            pltpu.VMEM((96, LANES), F32),
            pltpu.VMEM((96, LANES), F32),
            pltpu.VMEM((TRACEP, 4 * NE), F32),
            pltpu.VMEM((2 * TRACEP, 4 * NE), BF16),
            pltpu.VMEM((nslots_pad, 4 * NE), BF16),
            pltpu.VMEM((nslots_pad, 4 * NE), BF16),
            pltpu.VMEM((4 * NE, 4 * NE), BF16),
            pltpu.VMEM((TRACE, 4 * NE), F32),
            pltpu.VMEM((TRACE, 4 * NE), F32),
            pltpu.VMEM((96, LANES), F32),
            pltpu.VMEM((2 * TRACE, nslots_pad), BF16),
            pltpu.VMEM((2, nslots_pad, TRACEP), F32),
            pltpu.VMEM((2, nslots_pad, TRACEP), F32),
            pltpu.SemaphoreType.DMA((4,)),
            pltpu.SemaphoreType.DMA((2, 2 + ns)),
            pltpu.SemaphoreType.DMA((2, 2 + ns)),
        ]
        out = pl.pallas_call(
            functools.partial(kernel, nd, ns),
            out_shape=jax.ShapeDtypeStruct((NQ, NB, NE), F32),
            in_specs=[hbm] * 4 + [vmem] * 10,
            out_specs=vmem,
            scratch_shapes=scratch,
            compiler_params=pltpu.CompilerParams(
                collective_id=0, has_side_effects=True, vmem_limit_bytes=56 * 1024 * 1024
            ),
            name="ader_step",
        )(
            jnp.transpose(dof_values, (1, 0, 2)),
            jnp.transpose(star_matrices, (1, 2, 0, 3)),
            jnp.transpose(flux_local, (1, 2, 0, 3)),
            jnp.transpose(flux_neighbour, (1, 2, 0, 3)),
            stiffness,
            jnp.transpose(face_project, (1, 0, 2)),
            jnp.transpose(face_lift, (2, 0, 1)),
            face_rotate,
            cluster_labels.reshape(1, NE),
            neighbour_index,
            neighbour_face,
            neighbour_orient,
            send_element,
            send_face,
        )
        return jnp.transpose(out, (1, 0, 2))

    both = ("dom", "sub")
    in_specs = (
        P(None, None, both), P(), P(), P(), P(),
        P(None, None, None, both), P(None, None, None, both), P(None, None, None, both),
        P(both), P(None, both), P(None, both), P(None, both), P(both, None), P(both, None),
    )
    return jax.shard_map(
        per_device, mesh=mesh, in_specs=in_specs, out_specs=P(None, None, both), check_vma=False
    )
```

```python
import functools

import jax
import jax.numpy as jnp
from jax import lax
from jax.experimental import pallas as pl
from jax.experimental.pallas import tpu as pltpu
from jax.sharding import PartitionSpec as P

MESH = pl.DeviceIdType.MESH
F32, BF16 = jnp.float32, jnp.bfloat16
HIGHEST = lax.Precision.HIGHEST

NB = 56
NBP = 64
NQ = 9
NE = 128
NM = 21
NMP = 24
CURVE = 64
PEER = 8
TERMS = 6
LANES = NQ * NE
GROUP = 3
TRACE = 224
TRACEP = 256

NN = (((1,), (0,)), ((), ()))
NT = (((1,), (1,)), ((), ()))
TN = (((0,), (0,)), ((), ()))


def mm(a, b, dims=NN):
    return lax.dot_general(a, b, dims, preferred_element_type=F32)


def mm_exact(a, b, dims=NN):
    return lax.dot_general(a, b, dims, precision=HIGHEST, preferred_element_type=F32)


def iota(shape, dim):
    return lax.broadcasted_iota(jnp.int32, shape, dim)


def split(x):
    hi = x.astype(BF16)
    lo = (x - hi.astype(F32)).astype(BF16)
    return hi, lo


def row_block(index):
    out = jnp.zeros_like(index)
    for k in range(1, NQ):
        out = out + (index >= NMP * k).astype(jnp.int32)
    return out


def col(v):
    return slice(v * NE, (v + 1) * NE)


def kernel(
    nd, ns,
    dof_hbm, star_hbm, fluxl_hbm, fluxn_hbm,
    stiff_hbm, proj_hbm, lift_hbm, rot_hbm, labels_hbm, nidx_hbm, nface_hbm, norient_hbm,
    selem_hbm, sface_hbm,
    out,
    dof, star, fluxl, fluxn,
    stiff, proj, lift, rot, labels, nidx, nface, norient, selem, sface,
    starb, fluxlb, fluxnb,
    ader, avol, pst, lst, krc, tall,
    x, i1, i2, xs, z, vol, pi1, pi, t2, t2m, ohs, ohr, oho, zown, zr1, sol, rotm,
    send, recv,
    in_sem, send_sem, recv_sem,
):
    a = lax.axis_index("dom")
    b = lax.axis_index("sub")
    nslots = 2 * CURVE + PEER * ns

    barrier = pltpu.get_barrier_semaphore()

    @pl.when(a > 0)
    def _():
        pl.semaphore_signal(barrier, inc=1, device_id=(a - 1, b), device_id_type=MESH)

    @pl.when(a < nd - 1)
    def _():
        pl.semaphore_signal(barrier, inc=1, device_id=(a + 1, b), device_id_type=MESH)

    for o in range(1, ns):
        pl.semaphore_signal(barrier, inc=1, device_id=(a, lax.rem(b + o, ns)), device_id_type=MESH)

    copies = [
        pltpu.make_async_copy(src, dst, in_sem.at[k])
        for k, (src, dst) in enumerate(
            [
                (stiff_hbm, stiff), (proj_hbm, proj), (selem_hbm, selem), (sface_hbm, sface),
                (dof_hbm, dof), (star_hbm, star),
                (labels_hbm, labels), (lift_hbm, lift), (rot_hbm, rot), (nidx_hbm, nidx),
                (nface_hbm, nface), (norient_hbm, norient), (fluxl_hbm, fluxl), (fluxn_hbm, fluxn),
            ]
        )
    ]
    for c in copies:
        c.start()

    ohs[...] = jnp.zeros_like(ohs)
    t2[...] = jnp.zeros_like(t2)
    x[NB:, :] = jnp.zeros((NBP - NB, LANES), F32)
    i1[NB:, :] = jnp.zeros((NBP - NB, LANES), F32)
    i2[NB:, :] = jnp.zeros((NBP - NB, LANES), F32)

    def stacked(w):
        hi, lo = split(w)
        lane = iota(w.shape, 1)
        return jnp.where(lane < 2 * NBP, hi.astype(F32), lo.astype(F32)).astype(BF16)

    lane = iota((NB, 3 * NBP), 1)
    lane = lane - NBP * ((lane >= NBP).astype(jnp.int32) + (lane >= 2 * NBP).astype(jnp.int32))
    eye3 = (lane == iota((NB, 3 * NBP), 0)).astype(F32)

    for c in copies[0:4]:
        c.wait()

    def build_map(target, dims):
        tall[...] = jnp.zeros_like(tall)
        for d in range(3):
            tall[d * NB : (d + 1) * NB, :] = mm_exact(stiff[d], eye3, dims)
        target[...] = stacked(tall[0:176, :])

    build_map(ader, TN)
    for f in range(4):
        pi[f * NMP : (f + 1) * NMP, :] = jnp.zeros((NMP, LANES), F32)
        pi[f * NMP : f * NMP + NM, 0:NB] = proj[:, f, :]
    pst[...] = stacked(mm_exact(pi[0:96, 0:NB], eye3))

    diagonal = iota((nslots, nslots), 0) == iota((nslots, nslots), 1)
    ones = jnp.ones((nslots, NE), BF16)

    def as_column(row):
        spread = jnp.where(diagonal, jnp.broadcast_to(row.astype(F32), diagonal.shape), 0.0)
        return mm(spread.astype(BF16), ones)

    elem_col = as_column(selem[...])
    face_col = as_column(sface[...])
    lane_e = iota((nslots, NE), 1).astype(F32)
    for f in range(4):
        pick = (elem_col == lane_e) & (face_col == float(f))
        ohs[0:nslots, col(f)] = pick.astype(F32).astype(BF16)

    blank = jnp.zeros((CURVE, TRACEP), F32)
    for ex in range(2):
        @pl.when(a == 0)
        def _():
            recv[ex, 0:CURVE, :] = blank

        @pl.when(a == nd - 1)
        def _():
            recv[ex, CURVE : 2 * CURVE, :] = blank

        recv[ex, nslots:, :] = jnp.zeros((recv.shape[1] - nslots, TRACEP), F32)

    copies[4].wait()
    copies[5].wait()
    for v in range(NQ):
        for w in range(NQ):
            for d in range(3):
                starb[v, w, d] = jnp.broadcast_to(star[v, w, d : d + 1, :], (8, NE))

    def load_xs(value):
        hi, lo = split(value)
        xs[0:NBP, :] = hi
        xs[NBP : 2 * NBP, :] = lo
        xs[2 * NBP : 3 * NBP, :] = hi

    def mapped(matrix, target):
        z[0] = mm(matrix[...], xs[...])

        def group(g, carry):
            acc = [None] * GROUP
            for v in range(NQ):
                for d in range(3):
                    zb = z[0, d * NB : (d + 1) * NB, col(v)].reshape(NB // 8, 8, NE)
                    for k in range(GROUP):
                        term = zb * starb[v, g * GROUP + k, d][None]
                        acc[k] = term if acc[k] is None else acc[k] + term
            for k in range(GROUP):
                here = pl.ds(pl.multiple_of((g * GROUP + k) * NE, NE), NE)
                target[0:NB, here] = acc[k].reshape(NB, NE)
            return carry

        lax.fori_loop(0, NQ // GROUP, group, 0)

    def spread(values):
        hi, lo = split(values)
        return mm(ader[...], jnp.concatenate([hi, lo, hi], axis=0))

    def taylor(integrals):
        wide = GROUP * NE
        last = NQ - GROUP
        z[0, :, 0 : last * NE] = spread(x[:, 0 : last * NE])

        def step(t, carry):
            k = lax.div(t, 3)
            g = lax.rem(t, 3)
            behind = pl.ds(pl.multiple_of(lax.rem(g + 2, 3) * wide, NE), wide)
            now = lax.rem(k, 2)
            into = lax.rem(k + jnp.minimum(g, 1), 2)
            made = spread(x[:, behind])
            acc = [None] * GROUP
            for v in range(NQ):
                if v == last:
                    z[into, :, behind] = made
                for d in range(3):
                    zb = z[now, d * NB : (d + 1) * NB, col(v)].reshape(NB // 8, 8, NE)
                    for j in range(GROUP):
                        term = zb * starb[v, g * GROUP + j, d][None]
                        acc[j] = term if acc[j] is None else acc[j] + term
            for j in range(GROUP):
                here = pl.ds(pl.multiple_of((g * GROUP + j) * NE, NE), NE)
                value = acc[j].reshape(NB, NE)
                x[0:NB, here] = value
                for ref, table in integrals:
                    ref[0:NB, here] = ref[0:NB, here] + coefficient(k + 1, table) * value
            return carry

        lax.fori_loop(0, 3 * (TERMS - 1), step, 0)

    first_c, second_c = [1.0], [1.0]
    fact = 1.0
    for k in range(1, TERMS):
        fact *= k + 1
        first_c.append(1.0 / fact)
        second_c.append((2.0 ** (k + 1) - 1.0) / fact)

    def coefficient(k, table):
        out_c = jnp.float32(table[-1])
        for j in range(TERMS - 2, 0, -1):
            out_c = jnp.where(k == j, jnp.float32(table[j]), out_c)
        return out_c

    copies[6].wait()
    fine_row = labels[...] == 0
    fine = jnp.broadcast_to(fine_row, (NB, NE))

    for v in range(NQ):
        x[0:NB, col(v)] = dof[v]
    i1[...] = x[...]
    i2[...] = x[...]

    taylor([(i1, first_c), (i2, second_c)])

    def project(integral):
        load_xs(integral)
        pi[...] = mm(pst[...], xs[...])
        for f in range(4):
            for v in range(NQ):
                t2[v * NMP : (v + 1) * NMP, col(f)] = pi[f * NMP : (f + 1) * NMP, col(v)]
        hi, lo = split(t2[...])
        t2m[0:TRACEP, :] = hi
        t2m[TRACEP:, :] = lo

    def curve_copy(ex, up):
        src = pl.ds(CURVE if up else 0, CURVE)
        dst = pl.ds(0 if up else CURVE, CURVE)
        return pltpu.make_async_remote_copy(
            src_ref=send.at[ex, src, :],
            dst_ref=recv.at[ex, dst, :],
            send_sem=send_sem.at[ex, 0 if up else 1],
            recv_sem=recv_sem.at[ex, 0 if up else 1],
            device_id=(a + 1 if up else a - 1, b),
            device_id_type=MESH,
        )

    def peer_rows(p):
        return pl.ds(pl.multiple_of(2 * CURVE + p * PEER, PEER), PEER)

    def peer_copy(ex, p, source):
        return pltpu.make_async_remote_copy(
            src_ref=send.at[ex, peer_rows(p), :],
            dst_ref=recv.at[ex, peer_rows(source), :],
            send_sem=send_sem.at[ex, 2 + p],
            recv_sem=recv_sem.at[ex, 2 + source],
            device_id=(a, p),
            device_id_type=MESH,
        )

    order = sorted(range(1, ns), key=lambda o: -min(o, ns - o))

    def start_exchange(ex):
        both = mm(ohs[...], t2m[...], NT)
        send[ex] = both[:, 0:TRACEP] + both[:, TRACEP:]
        if ex == 0:
            count = ns - 1 + (a > 0).astype(jnp.int32) + (a < nd - 1).astype(jnp.int32)
            pl.semaphore_wait(barrier, count)
        for o in order:
            p = lax.rem(b + o, ns)
            peer_copy(ex, p, b).start()

        @pl.when(a < nd - 1)
        def _():
            curve_copy(ex, True).start()

        @pl.when(a > 0)
        def _():
            curve_copy(ex, False).start()

        recv[ex, peer_rows(b), :] = send[ex, peer_rows(b), :]

    def finish_exchange(ex):
        @pl.when(a > 0)
        def _():
            curve_copy(ex, True).wait_recv()

        @pl.when(a < nd - 1)
        def _():
            curve_copy(ex, False).wait_recv()

        for o in order:
            p = lax.rem(b + o, ns)
            peer_copy(ex, p, p).wait_recv()

    def finish_sends(ex):
        @pl.when(a < nd - 1)
        def _():
            curve_copy(ex, True).wait_send()

        @pl.when(a > 0)
        def _():
            curve_copy(ex, False).wait_send()

        for o in order:
            p = lax.rem(b + o, ns)
            peer_copy(ex, p, p).wait_send()

    def rotated_own(slot):
        picked = mm(t2m[...], oho[...])
        picked = picked[0:TRACEP, :] + picked[TRACEP:, :]
        hi, lo = split(picked)
        turned = mm(krc[...], jnp.concatenate([hi, lo, hi], axis=0))
        for f in range(4):
            orient = norient[f : f + 1, :]
            pick = jnp.where(
                orient == 0,
                turned[0:TRACE, col(f)],
                jnp.where(orient == 1, turned[TRACE : 2 * TRACE, col(f)], turned[2 * TRACE :, col(f)]),
            )
            if slot == 1:
                pick = pick + jnp.where(fine_row, 0.0, zr1[:, col(f)])
            zown[:, col(f)] = pick

    def local_flux():
        for f in range(4):
            for w0 in range(0, NQ, 3):
                acc = [None, None, None]
                for v in range(NQ):
                    block = pi[f * NMP : (f + 1) * NMP, col(v)].reshape(NMP // 8, 8, NE)
                    for k in range(3):
                        term = block * fluxlb[v, w0 + k, f][None]
                        acc[k] = term if acc[k] is None else acc[k] + term
                for k in range(3):
                    sol[f * NMP : (f + 1) * NMP, col(w0 + k)] = acc[k].reshape(NMP, NE)

    def remote_flux(slot_orient, ex):
        hi, lo = split(recv[ex])
        turned = mm(krc[...], jnp.concatenate([hi, lo, hi], axis=1), NT)
        pick = jnp.where(
            slot_orient < 0.5,
            turned[0:TRACE],
            jnp.where(slot_orient < 1.5, turned[TRACE : 2 * TRACE], turned[2 * TRACE :]),
        )
        hi, lo = split(pick)
        rotm[0:TRACE, :] = hi
        rotm[TRACE:, :] = lo
        arrived = mm(rotm[...], ohr[...])
        zown[...] = zown[...] + arrived[0:TRACE] + arrived[TRACE:]
        for f in range(4):
            for w0 in range(0, NQ, 3):
                acc = [
                    sol[f * NMP : (f + 1) * NMP, col(w0 + k)].reshape(NMP // 8, 8, NE) for k in range(3)
                ]
                for v in range(NQ):
                    block = zown[v * NMP : (v + 1) * NMP, col(f)].reshape(NMP // 8, 8, NE)
                    for k in range(3):
                        acc[k] = acc[k] + block * fluxnb[v, w0 + k, f][None]
                for k in range(3):
                    sol[f * NMP : (f + 1) * NMP, col(w0 + k)] = acc[k].reshape(NMP, NE)
        hi, lo = split(sol[...])
        lifted = mm(lst[...], jnp.concatenate([hi, lo], axis=0))
        vol[...] = vol[...] - lifted[0:NB] - lifted[NBP : NBP + NB]

    project(i1[...])
    start_exchange(0)

    build_map(avol, NN)
    for c in copies[7:]:
        c.wait()
    for v in range(NQ):
        for w in range(NQ):
            for f in range(4):
                fluxlb[v, w, f] = jnp.broadcast_to(fluxl[v, w, f : f + 1, :], (8, NE))
                fluxnb[v, w, f] = jnp.broadcast_to(fluxn[v, w, f : f + 1, :], (8, NE))

    tall[...] = jnp.zeros_like(tall)
    for f in range(4):
        tall[f * NMP : f * NMP + NM, 0:NB] = lift[:, f, :]
    lane2 = iota((96, 192), 1)
    lane2 = lane2 - 96 * (lane2 >= 96).astype(jnp.int32)
    eye2 = (lane2 == iota((96, 192), 0)).astype(F32)
    wide = mm_exact(tall[0:96, 0:NBP], eye2, TN)
    hi, lo = split(wide)
    lst[0:NBP, :] = hi
    lst[NBP:, :] = lo

    rows = iota((TRACEP, NM), 0)
    tile_of = ((rows - NMP * row_block(rows)) == iota((TRACEP, NM), 1)).astype(F32)
    tile_of = jnp.where(rows < NQ * NMP, tile_of, 0.0)
    same = row_block(iota((TRACE, TRACEP), 0)) == row_block(iota((TRACE, TRACEP), 1))
    for o in range(3):
        turned = mm_exact(tile_of[0:TRACE], rot[o])
        turned = jnp.where(same, mm_exact(turned, tile_of, NT), 0.0)
        hi, lo = split(turned)
        here = slice(o * TRACE, (o + 1) * TRACE)
        krc[here, 0:TRACEP] = hi
        krc[here, TRACEP : 2 * TRACEP] = hi
        krc[here, 2 * TRACEP :] = lo

    nslot_rows = ohr.shape[0]
    for f in range(4):
        index = nidx[f : f + 1, :]
        ohr[:, col(f)] = (iota((nslot_rows, NE), 0) + NE == index).astype(F32).astype(BF16)
        own = jnp.where(index < NE, nface[f : f + 1, :] * NE + index, -1)
        oho[:, col(f)] = (iota((4 * NE, NE), 0) == own).astype(F32).astype(BF16)

    slot_orient = mm(
        jnp.concatenate(
            [jnp.broadcast_to(norient[f : f + 1, :].astype(F32), (16, NE)) for f in range(4)], axis=1
        ).astype(BF16),
        ohr[...],
        NT,
    )[0:1, :]

    rotated_own(0)
    local_flux()
    pi1[...] = pi[...]
    mapped(avol, vol)

    finish_exchange(0)
    remote_flux(slot_orient, 0)
    zr1[...] = zown[...]

    for v in range(NQ):
        x[0:NB, col(v)] = dof[v] + jnp.where(fine, vol[:, col(v)], 0.0)
        dof[v] = x[0:NB, col(v)]
    vol[...] = x[0:NB]
    taylor([(vol, first_c)])
    for v in range(NQ):
        later = jnp.where(fine, vol[:, col(v)], i2[0:NB, col(v)])
        i1[0:NB, col(v)] = later + jnp.where(fine, 0.0, i1[0:NB, col(v)])
        i2[0:NB, col(v)] = later

    project(i2[...])
    start_exchange(1)

    for v in range(NQ):
        pi[:, col(v)] = pi[:, col(v)] + jnp.where(fine_row, 0.0, pi1[:, col(v)])
    rotated_own(1)
    local_flux()
    load_xs(i1[...])
    mapped(avol, vol)

    finish_exchange(1)
    remote_flux(slot_orient, 1)
    for v in range(NQ):
        out[v] = dof[v] + vol[:, col(v)]
    finish_sends(0)
    finish_sends(1)


def solution(mesh):
    nd, ns = mesh.shape["dom"], mesh.shape["sub"]
    nslots = 2 * CURVE + PEER * ns
    nslots_pad = -(-nslots // 128) * 128

    def per_device(
        dof_values, stiffness, face_project, face_lift, face_rotate, star_matrices,
        flux_local, flux_neighbour, cluster_labels, neighbour_index, neighbour_face,
        neighbour_orient, send_element, send_face,
    ):
        hbm = pl.BlockSpec(memory_space=pl.ANY)
        vmem = pl.BlockSpec(memory_space=pltpu.VMEM)
        scratch = [
            pltpu.VMEM((NQ, NB, NE), F32),
            pltpu.VMEM((NQ, NQ, 3, NE), F32),
            pltpu.VMEM((NQ, NQ, 4, NE), F32),
            pltpu.VMEM((NQ, NQ, 4, NE), F32),
            pltpu.VMEM((3, NB, NB), F32),
            pltpu.VMEM((NM, 4, NB), F32),
            pltpu.VMEM((NM, 4, NB), F32),
            pltpu.VMEM((3, NM, NM), F32),
            pltpu.VMEM((1, NE), jnp.int32),
            pltpu.VMEM((4, NE), jnp.int32),
            pltpu.VMEM((4, NE), jnp.int32),
            pltpu.VMEM((4, NE), jnp.int32),
            pltpu.VMEM((1, nslots), jnp.int32),
            pltpu.VMEM((1, nslots), jnp.int32),
            pltpu.VMEM((NQ, NQ, 3, 8, NE), F32),
            pltpu.VMEM((NQ, NQ, 4, 8, NE), F32),
            pltpu.VMEM((NQ, NQ, 4, 8, NE), F32),
            pltpu.VMEM((176, 3 * NBP), BF16),
            pltpu.VMEM((176, 3 * NBP), BF16),
            pltpu.VMEM((96, 3 * NBP), BF16),
            pltpu.VMEM((2 * NBP, 192), BF16),
            pltpu.VMEM((3 * TRACE, 3 * TRACEP), BF16),
            pltpu.VMEM((176, 3 * NBP), F32),
            pltpu.VMEM((NBP, LANES), F32),
            pltpu.VMEM((NBP, LANES), F32),
            pltpu.VMEM((NBP, LANES), F32),
            pltpu.VMEM((3 * NBP, LANES), BF16),
            pltpu.VMEM((2, 176, LANES), F32),
            pltpu.VMEM((NB, LANES), F32),
            pltpu.VMEM((96, LANES), F32),
            pltpu.VMEM((96, LANES), F32),
            pltpu.VMEM((TRACEP, 4 * NE), F32),
            pltpu.VMEM((2 * TRACEP, 4 * NE), BF16),
            pltpu.VMEM((nslots_pad, 4 * NE), BF16),
            pltpu.VMEM((nslots_pad, 4 * NE), BF16),
            pltpu.VMEM((4 * NE, 4 * NE), BF16),
            pltpu.VMEM((TRACE, 4 * NE), F32),
            pltpu.VMEM((TRACE, 4 * NE), F32),
            pltpu.VMEM((96, LANES), F32),
            pltpu.VMEM((2 * TRACE, nslots_pad), BF16),
            pltpu.VMEM((2, nslots_pad, TRACEP), F32),
            pltpu.VMEM((2, nslots_pad, TRACEP), F32),
            pltpu.SemaphoreType.DMA((14,)),
            pltpu.SemaphoreType.DMA((2, 2 + ns)),
            pltpu.SemaphoreType.DMA((2, 2 + ns)),
        ]
        out = pl.pallas_call(
            functools.partial(kernel, nd, ns),
            out_shape=pltpu.VMEM((NQ, NB, NE), F32),
            in_specs=[hbm] * 14,
            out_specs=vmem,
            scratch_shapes=scratch,
            compiler_params=pltpu.CompilerParams(
                collective_id=0, has_side_effects=True, vmem_limit_bytes=56 * 1024 * 1024
            ),
            name="ader_step",
        )(
            jnp.transpose(dof_values, (1, 0, 2)),
            jnp.transpose(star_matrices, (1, 2, 0, 3)),
            jnp.transpose(flux_local, (1, 2, 0, 3)),
            jnp.transpose(flux_neighbour, (1, 2, 0, 3)),
            stiffness,
            jnp.transpose(face_project, (1, 0, 2)),
            jnp.transpose(face_lift, (2, 0, 1)),
            face_rotate,
            cluster_labels.reshape(1, NE),
            neighbour_index,
            neighbour_face,
            neighbour_orient,
            send_element,
            send_face,
        )
        return jnp.transpose(out, (1, 0, 2))

    both = ("dom", "sub")
    in_specs = (
        P(None, None, both), P(), P(), P(), P(),
        P(None, None, None, both), P(None, None, None, both), P(None, None, None, both),
        P(both), P(None, both), P(None, both), P(None, both), P(both, None), P(both, None),
    )
    return jax.shard_map(
        per_device, mesh=mesh, in_specs=in_specs, out_specs=P(None, None, both), check_vma=False
    )
```

```python
import functools

import jax
import jax.numpy as jnp
from jax import lax
from jax.experimental import pallas as pl
from jax.experimental.pallas import tpu as pltpu
from jax.sharding import PartitionSpec as P

MESH = pl.DeviceIdType.MESH
F32, BF16 = jnp.float32, jnp.bfloat16
HIGHEST = lax.Precision.HIGHEST

NB = 56
NBP = 64
NQ = 9
NE = 128
NM = 21
NMP = 24
CURVE = 64
PEER = 8
TERMS = 6
LANES = NQ * NE
GROUP = 3
TRACE = 224
TRACEP = 256

NN = (((1,), (0,)), ((), ()))
NT = (((1,), (1,)), ((), ()))
TN = (((0,), (0,)), ((), ()))


def mm(a, b, dims=NN):
    return lax.dot_general(a, b, dims, preferred_element_type=F32)


def mm_exact(a, b, dims=NN):
    return lax.dot_general(a, b, dims, precision=HIGHEST, preferred_element_type=F32)


def iota(shape, dim):
    return lax.broadcasted_iota(jnp.int32, shape, dim)


def split(x):
    hi = x.astype(BF16)
    lo = (x - hi.astype(F32)).astype(BF16)
    return hi, lo


def row_block(index):
    out = jnp.zeros_like(index)
    for k in range(1, NQ):
        out = out + (index >= NMP * k).astype(jnp.int32)
    return out


def col(v):
    return slice(v * NE, (v + 1) * NE)


def kernel(
    nd, ns,
    dof_hbm, star_hbm, fluxl_hbm, fluxn_hbm,
    stiff_hbm, proj_hbm, lift_hbm, rot_hbm, labels_hbm, nidx_hbm, nface_hbm, norient_hbm,
    selem_hbm, sface_hbm,
    out,
    dof, star, fluxl, fluxn,
    stiff, proj, lift, rot, labels, nidx, nface, norient, selem, sface,
    starb, fluxlb, fluxnb,
    ader, avol, pst, lst, krc, tall,
    x, i1, i2, xs, z, vol, pi1, pi, t2, t2m, ohs, ohr, oho, zown, zr1, sol, rotm,
    send, recv,
    in_sem, send_sem, recv_sem,
):
    a = lax.axis_index("dom")
    b = lax.axis_index("sub")
    nslots = 2 * CURVE + PEER * ns

    barrier = pltpu.get_barrier_semaphore()

    @pl.when(a > 0)
    def _():
        pl.semaphore_signal(barrier, inc=1, device_id=(a - 1, b), device_id_type=MESH)

    @pl.when(a < nd - 1)
    def _():
        pl.semaphore_signal(barrier, inc=1, device_id=(a + 1, b), device_id_type=MESH)

    for o in range(1, ns):
        pl.semaphore_signal(barrier, inc=1, device_id=(a, lax.rem(b + o, ns)), device_id_type=MESH)

    copies = [
        pltpu.make_async_copy(src, dst, in_sem.at[k])
        for k, (src, dst) in enumerate(
            [
                (stiff_hbm, stiff), (proj_hbm, proj), (selem_hbm, selem), (sface_hbm, sface),
                (dof_hbm, dof), (star_hbm, star),
                (labels_hbm, labels), (lift_hbm, lift), (rot_hbm, rot), (nidx_hbm, nidx),
                (nface_hbm, nface), (norient_hbm, norient), (fluxl_hbm, fluxl), (fluxn_hbm, fluxn),
            ]
        )
    ]
    for c in copies:
        c.start()

    ohs[...] = jnp.zeros_like(ohs)
    t2[...] = jnp.zeros_like(t2)
    x[NB:, :] = jnp.zeros((NBP - NB, LANES), F32)
    i1[NB:, :] = jnp.zeros((NBP - NB, LANES), F32)
    i2[NB:, :] = jnp.zeros((NBP - NB, LANES), F32)

    def placed(w, high, low, dims=NN):
        hi, lo = split(w)
        return mm(hi.astype(F32), high, dims) + mm(lo.astype(F32), low, dims)

    lane = iota((NB, 3 * NBP), 1)
    row = iota((NB, 3 * NBP), 0)
    eye_high = ((lane == row) | (lane == row + NBP)).astype(F32)
    eye_low = (lane == row + 2 * NBP).astype(F32)

    for c in copies[0:4]:
        c.wait()

    def build_map(target, dims):
        tall[...] = jnp.zeros_like(tall)
        for d in range(3):
            tall[d * NB : (d + 1) * NB, :] = placed(stiff[d], eye_high, eye_low, dims)
        target[...] = tall[0:176, :].astype(BF16)

    build_map(ader, TN)
    for f in range(4):
        pi[f * NMP : (f + 1) * NMP, :] = jnp.zeros((NMP, LANES), F32)
        pi[f * NMP : f * NMP + NM, 0:NB] = proj[:, f, :]
    pst[...] = placed(pi[0:96, 0:NB], eye_high, eye_low).astype(BF16)

    diagonal = iota((nslots, nslots), 0) == iota((nslots, nslots), 1)
    ones = jnp.ones((nslots, NE), BF16)

    def as_column(row):
        spread = jnp.where(diagonal, jnp.broadcast_to(row.astype(F32), diagonal.shape), 0.0)
        return mm(spread.astype(BF16), ones)

    elem_col = as_column(selem[...])
    face_col = as_column(sface[...])
    lane_e = iota((nslots, NE), 1).astype(F32)
    for f in range(4):
        pick = (elem_col == lane_e) & (face_col == float(f))
        ohs[0:nslots, col(f)] = pick.astype(F32).astype(BF16)

    blank = jnp.zeros((CURVE, TRACEP), F32)
    for ex in range(2):
        @pl.when(a == 0)
        def _():
            recv[ex, 0:CURVE, :] = blank

        @pl.when(a == nd - 1)
        def _():
            recv[ex, CURVE : 2 * CURVE, :] = blank

        recv[ex, nslots:, :] = jnp.zeros((recv.shape[1] - nslots, TRACEP), F32)

    copies[4].wait()
    copies[5].wait()
    for v in range(NQ):
        for w in range(NQ):
            for d in range(3):
                starb[v, w, d] = jnp.broadcast_to(star[v, w, d : d + 1, :], (8, NE))

    def load_xs(value):
        hi, lo = split(value)
        xs[0:NBP, :] = hi
        xs[NBP : 2 * NBP, :] = lo
        xs[2 * NBP : 3 * NBP, :] = hi

    def mapped(matrix, target):
        z[0] = mm(matrix[...], xs[...])

        def group(g, carry):
            acc = [None] * GROUP
            for v in range(NQ):
                for d in range(3):
                    zb = z[0, d * NB : (d + 1) * NB, col(v)].reshape(NB // 8, 8, NE)
                    for k in range(GROUP):
                        term = zb * starb[v, g * GROUP + k, d][None]
                        acc[k] = term if acc[k] is None else acc[k] + term
            for k in range(GROUP):
                here = pl.ds(pl.multiple_of((g * GROUP + k) * NE, NE), NE)
                target[0:NB, here] = acc[k].reshape(NB, NE)
            return carry

        lax.fori_loop(0, NQ // GROUP, group, 0)

    def spread(values):
        hi, lo = split(values)
        return mm(ader[...], jnp.concatenate([hi, lo, hi], axis=0))

    def taylor(integrals):
        wide = GROUP * NE
        last = NQ - GROUP
        z[0, :, 0 : last * NE] = spread(x[:, 0 : last * NE])

        def step(t, carry):
            k = lax.div(t, 3)
            g = lax.rem(t, 3)
            behind = pl.ds(pl.multiple_of(lax.rem(g + 2, 3) * wide, NE), wide)
            now = lax.rem(k, 2)
            into = lax.rem(k + jnp.minimum(g, 1), 2)
            made = spread(x[:, behind])
            acc = [None] * GROUP
            for v in range(NQ):
                if v == last:
                    z[into, :, behind] = made
                for d in range(3):
                    zb = z[now, d * NB : (d + 1) * NB, col(v)].reshape(NB // 8, 8, NE)
                    for j in range(GROUP):
                        term = zb * starb[v, g * GROUP + j, d][None]
                        acc[j] = term if acc[j] is None else acc[j] + term
            for j in range(GROUP):
                here = pl.ds(pl.multiple_of((g * GROUP + j) * NE, NE), NE)
                value = acc[j].reshape(NB, NE)
                x[0:NB, here] = value
                for ref, table in integrals:
                    ref[0:NB, here] = ref[0:NB, here] + coefficient(k + 1, table) * value
            return carry

        lax.fori_loop(0, 3 * (TERMS - 1), step, 0, unroll=5)

    first_c, second_c = [1.0], [1.0]
    fact = 1.0
    for k in range(1, TERMS):
        fact *= k + 1
        first_c.append(1.0 / fact)
        second_c.append((2.0 ** (k + 1) - 1.0) / fact)

    def coefficient(k, table):
        out_c = jnp.float32(table[-1])
        for j in range(TERMS - 2, 0, -1):
            out_c = jnp.where(k == j, jnp.float32(table[j]), out_c)
        return out_c

    copies[6].wait()
    fine_row = labels[...] == 0
    fine = jnp.broadcast_to(fine_row, (NB, NE))

    for v in range(NQ):
        x[0:NB, col(v)] = dof[v]
    i1[...] = x[...]
    i2[...] = x[...]

    taylor([(i1, first_c), (i2, second_c)])

    def project(integral):
        load_xs(integral)
        pi[...] = mm(pst[...], xs[...])
        for f in range(4):
            for v in range(NQ):
                t2[v * NMP : (v + 1) * NMP, col(f)] = pi[f * NMP : (f + 1) * NMP, col(v)]
        hi, lo = split(t2[...])
        t2m[0:TRACEP, :] = hi
        t2m[TRACEP:, :] = lo

    def curve_copy(ex, up):
        src = pl.ds(CURVE if up else 0, CURVE)
        dst = pl.ds(0 if up else CURVE, CURVE)
        return pltpu.make_async_remote_copy(
            src_ref=send.at[ex, src, :],
            dst_ref=recv.at[ex, dst, :],
            send_sem=send_sem.at[ex, 0 if up else 1],
            recv_sem=recv_sem.at[ex, 0 if up else 1],
            device_id=(a + 1 if up else a - 1, b),
            device_id_type=MESH,
        )

    def peer_rows(p):
        return pl.ds(pl.multiple_of(2 * CURVE + p * PEER, PEER), PEER)

    def peer_copy(ex, p, source):
        return pltpu.make_async_remote_copy(
            src_ref=send.at[ex, peer_rows(p), :],
            dst_ref=recv.at[ex, peer_rows(source), :],
            send_sem=send_sem.at[ex, 2 + p],
            recv_sem=recv_sem.at[ex, 2 + source],
            device_id=(a, p),
            device_id_type=MESH,
        )

    order = sorted(range(1, ns), key=lambda o: -min(o, ns - o))

    def start_exchange(ex):
        both = mm(ohs[...], t2m[...], NT)
        send[ex] = both[:, 0:TRACEP] + both[:, TRACEP:]
        if ex == 0:
            count = ns - 1 + (a > 0).astype(jnp.int32) + (a < nd - 1).astype(jnp.int32)
            pl.semaphore_wait(barrier, count)
        for o in order:
            p = lax.rem(b + o, ns)
            peer_copy(ex, p, b).start()

        @pl.when(a < nd - 1)
        def _():
            curve_copy(ex, True).start()

        @pl.when(a > 0)
        def _():
            curve_copy(ex, False).start()

        recv[ex, peer_rows(b), :] = send[ex, peer_rows(b), :]

    def finish_exchange(ex):
        @pl.when(a > 0)
        def _():
            curve_copy(ex, True).wait_recv()

        @pl.when(a < nd - 1)
        def _():
            curve_copy(ex, False).wait_recv()

        for o in order:
            p = lax.rem(b + o, ns)
            peer_copy(ex, p, p).wait_recv()

    def finish_sends(ex):
        @pl.when(a < nd - 1)
        def _():
            curve_copy(ex, True).wait_send()

        @pl.when(a > 0)
        def _():
            curve_copy(ex, False).wait_send()

        for o in order:
            p = lax.rem(b + o, ns)
            peer_copy(ex, p, p).wait_send()

    def rotated_own(slot):
        picked = mm(t2m[...], oho[...])
        picked = picked[0:TRACEP, :] + picked[TRACEP:, :]
        hi, lo = split(picked)
        turned = mm(krc[...], jnp.concatenate([hi, lo, hi], axis=0))
        for f in range(4):
            orient = norient[f : f + 1, :]
            pick = jnp.where(
                orient == 0,
                turned[0:TRACE, col(f)],
                jnp.where(orient == 1, turned[TRACE : 2 * TRACE, col(f)], turned[2 * TRACE :, col(f)]),
            )
            if slot == 1:
                pick = pick + jnp.where(fine_row, 0.0, zr1[:, col(f)])
            zown[:, col(f)] = pick

    def local_flux():
        for f in range(4):
            for w0 in range(0, NQ, 3):
                acc = [None, None, None]
                for v in range(NQ):
                    block = pi[f * NMP : (f + 1) * NMP, col(v)].reshape(NMP // 8, 8, NE)
                    for k in range(3):
                        term = block * fluxlb[v, w0 + k, f][None]
                        acc[k] = term if acc[k] is None else acc[k] + term
                for k in range(3):
                    sol[f * NMP : (f + 1) * NMP, col(w0 + k)] = acc[k].reshape(NMP, NE)

    def remote_flux(slot_orient, ex):
        hi, lo = split(recv[ex])
        turned = mm(krc[...], jnp.concatenate([hi, lo, hi], axis=1), NT)
        pick = jnp.where(
            slot_orient < 0.5,
            turned[0:TRACE],
            jnp.where(slot_orient < 1.5, turned[TRACE : 2 * TRACE], turned[2 * TRACE :]),
        )
        hi, lo = split(pick)
        rotm[0:TRACE, :] = hi
        rotm[TRACE:, :] = lo
        arrived = mm(rotm[...], ohr[...])
        zown[...] = zown[...] + arrived[0:TRACE] + arrived[TRACE:]
        for f in range(4):
            for w0 in range(0, NQ, 3):
                acc = [
                    sol[f * NMP : (f + 1) * NMP, col(w0 + k)].reshape(NMP // 8, 8, NE) for k in range(3)
                ]
                for v in range(NQ):
                    block = zown[v * NMP : (v + 1) * NMP, col(f)].reshape(NMP // 8, 8, NE)
                    for k in range(3):
                        acc[k] = acc[k] + block * fluxnb[v, w0 + k, f][None]
                for k in range(3):
                    sol[f * NMP : (f + 1) * NMP, col(w0 + k)] = acc[k].reshape(NMP, NE)
        hi, lo = split(sol[...])
        lifted = mm(lst[...], jnp.concatenate([hi, lo], axis=0))
        vol[...] = vol[...] - lifted[0:NB] - lifted[NBP : NBP + NB]

    project(i1[...])
    start_exchange(0)

    build_map(avol, NN)
    for c in copies[7:]:
        c.wait()
    for v in range(NQ):
        for w in range(NQ):
            for f in range(4):
                fluxlb[v, w, f] = jnp.broadcast_to(fluxl[v, w, f : f + 1, :], (8, NE))
                fluxnb[v, w, f] = jnp.broadcast_to(fluxn[v, w, f : f + 1, :], (8, NE))

    tall[...] = jnp.zeros_like(tall)
    for f in range(4):
        tall[f * NMP : f * NMP + NM, 0:NB] = lift[:, f, :]
    lane2 = iota((96, 192), 1)
    lane2 = lane2 - 96 * (lane2 >= 96).astype(jnp.int32)
    eye2 = (lane2 == iota((96, 192), 0)).astype(F32)
    wide = mm_exact(tall[0:96, 0:NBP], eye2, TN)
    hi, lo = split(wide)
    lst[0:NBP, :] = hi
    lst[NBP:, :] = lo

    rows = iota((TRACEP, NM), 0)
    tile_of = ((rows - NMP * row_block(rows)) == iota((TRACEP, NM), 1)).astype(F32)
    tile_of = jnp.where(rows < NQ * NMP, tile_of, 0.0)
    same = row_block(iota((TRACE, TRACEP), 0)) == row_block(iota((TRACE, TRACEP), 1))
    for o in range(3):
        turned = mm_exact(tile_of[0:TRACE], rot[o])
        turned = jnp.where(same, mm_exact(turned, tile_of, NT), 0.0)
        hi, lo = split(turned)
        here = slice(o * TRACE, (o + 1) * TRACE)
        krc[here, 0:TRACEP] = hi
        krc[here, TRACEP : 2 * TRACEP] = hi
        krc[here, 2 * TRACEP :] = lo

    nslot_rows = ohr.shape[0]
    for f in range(4):
        index = nidx[f : f + 1, :]
        ohr[:, col(f)] = (iota((nslot_rows, NE), 0) + NE == index).astype(F32).astype(BF16)
        own = jnp.where(index < NE, nface[f : f + 1, :] * NE + index, -1)
        oho[:, col(f)] = (iota((4 * NE, NE), 0) == own).astype(F32).astype(BF16)

    slot_orient = mm(
        jnp.concatenate(
            [jnp.broadcast_to(norient[f : f + 1, :].astype(F32), (16, NE)) for f in range(4)], axis=1
        ).astype(BF16),
        ohr[...],
        NT,
    )[0:1, :]

    rotated_own(0)
    local_flux()
    pi1[...] = pi[...]
    mapped(avol, vol)

    finish_exchange(0)
    remote_flux(slot_orient, 0)
    zr1[...] = zown[...]

    for v in range(NQ):
        x[0:NB, col(v)] = dof[v] + jnp.where(fine, vol[:, col(v)], 0.0)
        dof[v] = x[0:NB, col(v)]
    vol[...] = x[0:NB]
    taylor([(vol, first_c)])
    for v in range(NQ):
        later = jnp.where(fine, vol[:, col(v)], i2[0:NB, col(v)])
        i1[0:NB, col(v)] = later + jnp.where(fine, 0.0, i1[0:NB, col(v)])
        i2[0:NB, col(v)] = later

    project(i2[...])
    start_exchange(1)

    for v in range(NQ):
        pi[:, col(v)] = pi[:, col(v)] + jnp.where(fine_row, 0.0, pi1[:, col(v)])
    rotated_own(1)
    local_flux()
    load_xs(i1[...])
    mapped(avol, vol)

    finish_exchange(1)
    remote_flux(slot_orient, 1)
    for v in range(NQ):
        out[v] = dof[v] + vol[:, col(v)]
    finish_sends(0)
    finish_sends(1)


def solution(mesh):
    nd, ns = mesh.shape["dom"], mesh.shape["sub"]
    nslots = 2 * CURVE + PEER * ns
    nslots_pad = -(-nslots // 128) * 128

    def per_device(
        dof_values, stiffness, face_project, face_lift, face_rotate, star_matrices,
        flux_local, flux_neighbour, cluster_labels, neighbour_index, neighbour_face,
        neighbour_orient, send_element, send_face,
    ):
        hbm = pl.BlockSpec(memory_space=pl.ANY)
        vmem = pl.BlockSpec(memory_space=pltpu.VMEM)
        scratch = [
            pltpu.VMEM((NQ, NB, NE), F32),
            pltpu.VMEM((NQ, NQ, 3, NE), F32),
            pltpu.VMEM((NQ, NQ, 4, NE), F32),
            pltpu.VMEM((NQ, NQ, 4, NE), F32),
            pltpu.VMEM((3, NB, NB), F32),
            pltpu.VMEM((NM, 4, NB), F32),
            pltpu.VMEM((NM, 4, NB), F32),
            pltpu.VMEM((3, NM, NM), F32),
            pltpu.VMEM((1, NE), jnp.int32),
            pltpu.VMEM((4, NE), jnp.int32),
            pltpu.VMEM((4, NE), jnp.int32),
            pltpu.VMEM((4, NE), jnp.int32),
            pltpu.VMEM((1, nslots), jnp.int32),
            pltpu.VMEM((1, nslots), jnp.int32),
            pltpu.VMEM((NQ, NQ, 3, 8, NE), F32),
            pltpu.VMEM((NQ, NQ, 4, 8, NE), F32),
            pltpu.VMEM((NQ, NQ, 4, 8, NE), F32),
            pltpu.VMEM((176, 3 * NBP), BF16),
            pltpu.VMEM((176, 3 * NBP), BF16),
            pltpu.VMEM((96, 3 * NBP), BF16),
            pltpu.VMEM((2 * NBP, 192), BF16),
            pltpu.VMEM((3 * TRACE, 3 * TRACEP), BF16),
            pltpu.VMEM((176, 3 * NBP), F32),
            pltpu.VMEM((NBP, LANES), F32),
            pltpu.VMEM((NBP, LANES), F32),
            pltpu.VMEM((NBP, LANES), F32),
            pltpu.VMEM((3 * NBP, LANES), BF16),
            pltpu.VMEM((2, 176, LANES), F32),
            pltpu.VMEM((NB, LANES), F32),
            pltpu.VMEM((96, LANES), F32),
            pltpu.VMEM((96, LANES), F32),
            pltpu.VMEM((TRACEP, 4 * NE), F32),
            pltpu.VMEM((2 * TRACEP, 4 * NE), BF16),
            pltpu.VMEM((nslots_pad, 4 * NE), BF16),
            pltpu.VMEM((nslots_pad, 4 * NE), BF16),
            pltpu.VMEM((4 * NE, 4 * NE), BF16),
            pltpu.VMEM((TRACE, 4 * NE), F32),
            pltpu.VMEM((TRACE, 4 * NE), F32),
            pltpu.VMEM((96, LANES), F32),
            pltpu.VMEM((2 * TRACE, nslots_pad), BF16),
            pltpu.VMEM((2, nslots_pad, TRACEP), F32),
            pltpu.VMEM((2, nslots_pad, TRACEP), F32),
            pltpu.SemaphoreType.DMA((14,)),
            pltpu.SemaphoreType.DMA((2, 2 + ns)),
            pltpu.SemaphoreType.DMA((2, 2 + ns)),
        ]
        out = pl.pallas_call(
            functools.partial(kernel, nd, ns),
            out_shape=pltpu.VMEM((NQ, NB, NE), F32),
            in_specs=[hbm] * 14,
            out_specs=vmem,
            scratch_shapes=scratch,
            compiler_params=pltpu.CompilerParams(
                collective_id=0, has_side_effects=True, vmem_limit_bytes=56 * 1024 * 1024
            ),
            name="ader_step",
        )(
            jnp.transpose(dof_values, (1, 0, 2)),
            jnp.transpose(star_matrices, (1, 2, 0, 3)),
            jnp.transpose(flux_local, (1, 2, 0, 3)),
            jnp.transpose(flux_neighbour, (1, 2, 0, 3)),
            stiffness,
            jnp.transpose(face_project, (1, 0, 2)),
            jnp.transpose(face_lift, (2, 0, 1)),
            face_rotate,
            cluster_labels.reshape(1, NE),
            neighbour_index,
            neighbour_face,
            neighbour_orient,
            send_element,
            send_face,
        )
        return jnp.transpose(out, (1, 0, 2))

    both = ("dom", "sub")
    in_specs = (
        P(None, None, both), P(), P(), P(), P(),
        P(None, None, None, both), P(None, None, None, both), P(None, None, None, both),
        P(both), P(None, both), P(None, both), P(None, both), P(both, None), P(both, None),
    )
    return jax.shard_map(
        per_device, mesh=mesh, in_specs=in_specs, out_specs=P(None, None, both), check_vma=False
    )
```
